32 devices in a mesh: gx: 4 (over y, core), yz: 8 (over z, x).
Axes of the slice: x: 2, y: 2, z: 4, core: 2. Of those that a mesh axis runs over, the one named last changes fastest.
Arguments:
- orbitals: bfloat16 [4, 8, 9, 128, 256], P('gx', 'yz'), may hold values from -0.125 to 0.125
- potential: float32 [4, 8, 256], P('gx', 'yz'), may hold values from 0.25 to 4
- density: bfloat16 [4, 8, 9, 128, 128], P('gx', 'yz'), may hold values from -0.1 to 0.6
- pattern: int32 [4, 8, 9], P('gx', 'yz'), may hold values 0 or 1
Outputs:
- hamiltonian: float32 [4, 8, 9, 128, 128], P('gx', 'yz')
- margin: float32 [4, 8, 9, 128, 128], P('gx', 'yz')
- purified: float32 [4, 8, 9, 128, 128], P('gx', 'yz')
The draws below stay inside these ranges and needn't reach their ends.
All inputs are finite; a program needn't handle non-finite values. No bound on the sum of `pattern` on one device may be relied on, other than what follows from the above.
Results may differ from the reference program's by a relative error of at most 0.0068.
Values may be sent and summed in bfloat16 or wider, within the bound.
A program may use at most 64 MiB of HBM per device.

```python
import math
import jax
import jax.numpy as jnp

BLK = 128
G_DEV = 256
NGX = 4
NYZ = 8


def draw_density(key, part):
    noise = 0.01 * jax.random.normal(key, (NGX, NYZ, 9, BLK, BLK), jnp.float32)
    identity = jnp.eye(BLK, dtype=jnp.float32)
    centre = (jnp.arange(9) == 4).astype(jnp.float32)
    return (noise + 0.5 * centre[None, None, :, None, None] * identity).astype(jnp.bfloat16)


def set_ends(array, rng, low, top_value):
    dims = array.shape
    index_at = [jax.random.randint(jax.random.fold_in(rng, axis), (), 0, dims[axis]) for axis in range(len(dims))]
    array = array.at[tuple(index_at)].set(low)
    longest = dims.index(max(dims))
    index_at[longest] = (index_at[longest] + 1) % dims[longest]
    return array.at[tuple(index_at)].set(top_value)


def block_levels(key, extent, split, least, top_value):
    level = 1.0
    for axis_at, blocks in split:
        heights = jax.random.uniform(jax.random.fold_in(jax.random.fold_in(key, 6), axis_at), (blocks,), jnp.float32, least / len(split), top_value / len(split))
        level = level * jnp.repeat(jnp.exp(heights), extent[axis_at] // blocks).reshape((-1,) + (1,) * (len(extent) - 1 - axis_at))
    return level


def centred(own_key, extent, width, bound, split=(), held_as=jnp.bfloat16):
    gain = block_levels(own_key, extent, split, -0.22, 0.18) if split else 1.0
    result = jax.random.normal(own_key, extent, jnp.float32) * width * gain
    return jnp.minimum(jnp.maximum(result, -bound), bound).astype(held_as)


def setup_inputs(seed: int = 0) -> dict:
    keys = jax.random.split(jax.random.key(seed), 5)
    return {
        "orbitals": centred(keys[0], (NGX, NYZ, 9, BLK, G_DEV), (9 * G_DEV) ** -0.5, 0.125, ((0, 4), (1, 8))),
        "potential": jnp.clip(jnp.exp(math.log(4.0) - 2.7725887 * jax.random.uniform(keys[1], (NGX, NYZ, G_DEV), jnp.float32) ** block_levels(keys[1], (NGX, NYZ, G_DEV), ((0, 4), (1, 8)), -0.2, 0.2)), 0.25, 4.0),
        "density": draw_density(jax.random.fold_in(keys[4], 71), 0),
        "pattern": set_ends((jax.random.randint(keys[3], (NGX, NYZ, 9), 0, 5) < 4).astype(jnp.int32), jax.random.fold_in(keys[3], 1), 0, 1),
    }


def offset_of(index):
    return index // 3 - 1, index % 3 - 1


def slot_for(shift_x, shift_y):
    return (shift_x + 1) * 3 + shift_y + 1


def line_steps(values):
    lead = values.shape[:-1]
    lines = values.astype(jnp.float32).reshape(lead + (values.shape[-1] // 128, 128))
    forward = lines[..., 1:] - lines[..., :-1]
    padded = jnp.concatenate([forward, jnp.zeros(lead + (lines.shape[-2], 1), jnp.float32)], axis=-1)
    return padded.reshape(values.shape).astype(jnp.bfloat16)


def block_product(left, right, keep):
    out = jnp.zeros(left.shape, jnp.float32)
    for first in range(9):
        fa, fb = offset_of(first)
        for second in range(9):
            sa, sb = offset_of(second)
            oa, ob = fa + sa, fb + sb
            if abs(oa) > 1 or abs(ob) > 1:
                continue
            moved = jnp.roll(right[:, :, second], (-fa, -fb), axis=(0, 1))
            term = jnp.einsum("xyij,xyjk->xyik", left[:, :, first].astype(jnp.float32), moved.astype(jnp.float32))
            out = out.at[:, :, slot_for(oa, ob)].add(term)
    return out * keep


def reference(orbitals, potential, density, pattern):
    keep = pattern.astype(jnp.float32)[:, :, :, None, None]
    weighted = (orbitals.astype(jnp.float32) * potential[:, :, None, None, :]).astype(jnp.bfloat16)
    steps = line_steps(orbitals)
    hamiltonian = jnp.zeros(density.shape, jnp.float32)
    margin = jnp.zeros(density.shape, jnp.float32)
    for slot in range(9):
        ka, kb = offset_of(slot)
        left = orbitals[:, :, slot].astype(jnp.float32)
        left_steps = steps[:, :, slot].astype(jnp.float32)
        for target in range(9):
            pa, pb = offset_of(target)
            la, lb = ka - pa, kb - pb
            if abs(la) > 1 or abs(lb) > 1:
                continue
            other = slot_for(la, lb)
            s_term = jnp.einsum("xyig,xyjg->xyij", left, orbitals[:, :, other].astype(jnp.float32))
            h_term = jnp.einsum("xyig,xyjg->xyij", left, weighted[:, :, other].astype(jnp.float32))
            h_term = h_term + 0.5 * jnp.einsum("xyig,xyjg->xyij", left_steps, steps[:, :, other].astype(jnp.float32))
            margin = margin.at[:, :, target].add(jnp.roll(s_term, (-ka, -kb), axis=(0, 1)))
            hamiltonian = hamiltonian.at[:, :, target].add(jnp.roll(h_term, (-ka, -kb), axis=(0, 1)))
    hamiltonian = hamiltonian * keep
    margin = margin * keep
    current = density * pattern.astype(jnp.bfloat16)[:, :, :, None, None]
    margin_low = margin.astype(jnp.bfloat16)
    purified = jnp.zeros(density.shape, jnp.float32)
    for step in range(2):
        first = block_product(current, margin_low, keep)
        first_low = first.astype(jnp.bfloat16)
        third = block_product(first_low, current, keep)
        third_low = third.astype(jnp.bfloat16)
        fifth = block_product(first_low, third_low, keep)
        purified = 3.0 * third - 2.0 * fifth
        current = purified.astype(jnp.bfloat16)
    return hamiltonian, margin, purified
```

```python
import functools

import jax
import jax.numpy as jnp
from jax import lax
from jax.experimental import pallas as pl
from jax.experimental.pallas import tpu as pltpu
from jax.sharding import PartitionSpec as P

MESH = pl.DeviceIdType.MESH
SPAN = (-1, 0, 1)
AROUND = [(a, b) for a in SPAN for b in SPAN if (a, b) != (0, 0)]
PORTS = 144


def part(d):
    return pl.ds(1, 2) if d == 1 else pl.ds(0, 2) if d == -1 else pl.ds(0, 3)


class Either:
    def __init__(self, copy, apart):
        self.copy, self.apart = copy, apart

    def wait_recv(self):
        pl.when(self.apart)(lambda: self.copy.wait_recv())

    def wait_send(self):
        pl.when(self.apart)(lambda: self.copy.wait_send())


class Wire:
    def __init__(self, send, recv):
        self.send, self.recv = send, recv
        self.ports = iter(range(PORTS))
        self.started = []

    def __call__(self, src, dst, device, apart=None):
        at = next(self.ports)
        copy = pltpu.make_async_remote_copy(
            src_ref=src, dst_ref=dst, send_sem=self.send.at[at], recv_sem=self.recv.at[at],
            device_id=device, device_id_type=MESH,
        )
        if apart is None:
            copy.start()
        else:
            pl.when(apart)(lambda: copy.start())

            @pl.when(jnp.logical_not(apart))
            def _():
                dst[...] = src[...]

            copy = Either(copy, apart)
        self.started.append(copy)
        return copy

    def drain(self):
        for copy in self.started:
            copy.wait_send()


class Places:
    def __init__(self, counts):
        self.counts = counts
        many = counts[1]
        self.table = list(range(many))
        if many % 2 == 0 and many >= 8:
            tall = many // 2
            self.table = [2, 0] + [2 * z + 1 for z in range(tall)] + [2 * z for z in range(tall - 1, 1, -1)]
        self.roles = [self.table.index(b) for b in range(many)]
        self.a, self.b = lax.axis_index("gx"), lax.axis_index("yz")
        self.c = self.pick(self.roles, self.b)
        self.outer = 2 * lax.rem(self.a, 2) - 1

    def pick(self, table, at):
        value = jnp.int32(table[0])
        for i in range(1, len(table)):
            value = jnp.where(at == i, jnp.int32(table[i]), value)
        return value

    def row(self, da):
        return lax.rem(self.a + da + self.counts[0], self.counts[0])

    def ring(self, b):
        return lax.rem(b + self.counts[1], self.counts[1])

    def seat(self, b):
        return self.pick(self.table, self.ring(b))

    def home(self, da, db):
        return self.row(da), self.ring(self.b + db)

    def near(self, da, db):
        return self.row(da), self.seat(self.c + db)

    def inward(self, db):
        return self.a, self.seat(self.b + db)

    def apart(self, db):
        return self.ring(self.b + db) != self.c

    def outward(self, da, db):
        return self.row(da), self.ring(self.c + db)

    def away(self, db):
        return self.ring(self.c + db) != self.b

    def greet(self, barrier):
        many = self.counts[1]
        lists = []
        for b in range(many):
            c, met = self.roles[b], set()
            for db in SPAN:
                met |= {(b + db) % many, self.table[(b + db) % many]}
                met |= {(c + db) % many, self.table[(c + db) % many]}
            lists.append(sorted(met - {b}))
        for at in range(max(len(met) for met in lists)):
            to = self.pick([met[at] if at < len(met) else -1 for met in lists], self.b)

            @pl.when(to >= 0)
            def _():
                for da in SPAN:
                    pl.semaphore_signal(
                        barrier, inc=1, device_id=(self.row(da), to), device_id_type=MESH
                    )

        for da in (1, -1):
            pl.semaphore_signal(barrier, inc=1, device_id=(self.row(da), self.b), device_id_type=MESH)
        return self.pick([3 * len(met) + 2 for met in lists], self.b)


class Halo:
    def __init__(self, wire, places, near, base=None, whole=False, split=False):
        self.wire, self.places, self.near, self.base = wire, places, near, base
        self.whole, self.split = whole, split
        outer = places.outer
        self.order = [
            (db, piece, pa, das)
            for piece, pa, das in (
                ((0, None, (1, -1)),) if whole else (
                    (0, 1, (outer, -outer)),
                    (2, 1 - outer, (-outer,)),
                    (1, 1 + outer, () if split else (outer,)),
                )
            )
            for db in ((1, -1) if base is None else (0, 1, -1))
        ]
        self.direct = {}
        self.passed = []

    def make(self, src, da, db, device, pa, apart=None):
        dst = self.near.at[1 - da, 1 - db]
        if not self.whole:
            src = src.at[pa, part(db)]
            dst = dst.at[pa, part(db)]
        return self.wire(src, dst, device, apart)

    def start_far(self, which=None):
        for db, piece, pa, _ in self.order:
            if which is not None and piece != which:
                continue
            if self.base is None:
                copy = self.make(self.near.at[1, 1], 0, db, self.places.near(0, db), pa)
            else:
                copy = self.make(self.base, 0, db, self.places.inward(db), pa, self.places.apart(db))
            self.direct[db, piece] = copy

    def start_near(self, name):
        outer = self.places.outer
        da, pa = {
            "turned": (outer, 1 + outer), "outer": (outer, 1),
            "inner": (-outer, 1), "last": (-outer, 1 - outer),
        }[name]
        self.direct[name] = self.make(self.near.at[1, 1], da, 0, self.places.near(da, 0), pa)

    def ready(self, at):
        if at == 0:
            self.start_near("turned")
        elif at == 1:
            self.start_far(0)
            self.start_near("outer")
            self.start_near("inner")
        else:
            self.start_far(2)
            self.start_far(1)
            self.start_near("last")

    def relay(self, start=0, stop=None):
        for db, piece, pa, das in self.order[start:stop]:
            if das:
                self.direct[db, piece].wait_recv()
            for at, da in enumerate(das):
                src = self.near.at[1, 1 - db]
                copy = self.make(src, da, db, self.places.near(da, 0), pa)
                self.passed.append((piece == 2 or at == 1, copy))

    def cross(self):
        outer = self.places.outer
        self.direct["turned"].wait_recv()
        for db in (1, -1):
            src = self.near.at[1 + outer, 1, 1 - outer, part(db)]
            dst = self.near.at[1 + outer, 1 - db, 1 - outer, part(db)]
            self.passed.append((False, self.wire(src, dst, self.places.near(0, db))))

    def finish_inner(self):
        for db, piece, _, das in self.order:
            if not das:
                self.direct[db, piece].wait_recv()
        for name in ("inner", "last"):
            self.direct[name].wait_recv()
        for inner, copy in self.passed:
            if inner:
                copy.wait_recv()

    def finish_outer(self):
        self.direct["outer"].wait_recv()
        for inner, copy in self.passed:
            if not inner:
                copy.wait_recv()

    def finish(self):
        for _, copy in self.passed:
            copy.wait_recv()


class Slim:
    def __init__(self, wire, places, near):
        self.wire, self.places, self.near = wire, places, near
        self.far, self.close, self.passed = {}, [], []

    def start_far(self):
        own = self.near.at[1, 1]
        for db in (1, -1):
            dst = self.near.at[1, 1 - db]
            self.far[db] = self.wire(
                own.at[pl.ds(0, 3), 1], dst.at[pl.ds(0, 3), 1], self.places.near(0, db)
            )

    def start_near(self):
        own = self.near.at[1, 1]
        for da in (1, -1):
            dst = self.near.at[1 - da, 1]
            to = self.places.near(da, 0)
            self.close.append(self.wire(own.at[1], dst.at[1], to))
            for pb in (0, 2):
                self.close.append(self.wire(own.at[1 + da, pb], dst.at[1 + da, pb], to))

    def relay(self):
        for db in (1, -1):
            self.far[db].wait_recv()
            for da in (1, -1):
                src = self.near.at[1, 1 - db, 1, 1]
                dst = self.near.at[1 - da, 1 - db, 1, 1]
                self.passed.append(self.wire(src, dst, self.places.near(da, 0)))

    def finish(self):
        for copy in self.close + self.passed:
            copy.wait_recv()

    @staticmethod
    def sent(ja, jb, pa, pb):
        if (pa, pb) == (0, 0):
            return True
        if ja == 0:
            return pb == 0
        return jb == 0 and pb != 0 and pa in (0, -ja)


def groups(outer):
    return ((outer, (0, outer)), (0, (0, outer, -outer)), (-outer, (0, -outer)))


def product(left, near, outer, emit, done):
    width = left.shape[-1]
    blank = jnp.zeros((width, width), jnp.bfloat16)
    for at, (pa, fas) in enumerate(groups(outer)):
        total = None
        for fa in fas:
            lhs = jnp.concatenate([left[fa + 1, fb + 1] for fb in SPAN], axis=1)
            rhs = jnp.concatenate([
                jnp.concatenate([
                    near[fa + 1, fb + 1, pa - fa + 1, pb - fb + 1] if abs(pb - fb) <= 1 else blank
                    for pb in SPAN
                ], axis=1) for fb in SPAN
            ], axis=0)
            term = jnp.dot(lhs, rhs, preferred_element_type=jnp.float32)
            total = term if total is None else total + term
        for pb in SPAN:
            emit(pa, pb, total[:, (pb + 1) * width:(pb + 2) * width])
        done(at)


def column(width, lefts, rights, turned, ka, fas, base=None):
    blank = jnp.zeros((width, width), jnp.bfloat16)
    inner = [(fa, fb) for fa in fas for fb in SPAN]
    lhs = jnp.concatenate([
        jnp.concatenate(
            [lefts((ka, kb), f) if abs(f[1] - kb) <= 1 else blank for f in inner], axis=1
        ) for kb in SPAN
    ], axis=0)
    rhs = jnp.concatenate([rights(f) for f in inner], axis=1 if turned else 0)
    total = lax.dot_general(
        lhs, rhs, (((1,), (1 if turned else 0,)), ((), ())), preferred_element_type=jnp.float32
    )
    return total if base is None else total + base


def give(width, ka, total, emit):
    for kb in SPAN:
        emit(ka, kb, total[(kb + 1) * width:(kb + 2) * width])


class Gram:
    A_PAIRS = ((0, 1, 1), (1, 1, 0), (4, -1, -1), (5, 0, -1), (8, 0, 0))
    B_PAIRS = ((2, 1, 1), (3, 1, 0), (6, -1, -1), (7, -1, 0), (9, 0, -1), (10, 0, 0), (11, 0, 1))
    MIDDLE = ((0, 8), (0, 5), (0, 1), (1, 9), (1, 10), (1, 11), (2, 9), (2, 10), (2, 11))
    CHUNKS = (pl.ds(0, 4), pl.ds(4, 4), pl.ds(8, 4))

    def __init__(self, wire, places, lefts, rights, own, out, into, out_far, into_far, out_mid=None, into_mid=None):
        self.wire, self.places, self.outer = wire, places, places.outer
        self.lefts, self.rights = lefts, rights
        self.own, self.out, self.into, self.out_far, self.into_far = own, out, into, out_far, into_far
        self.out_mid, self.into_mid = out_mid, into_mid
        self.width = lefts.shape[2]
        self.first = {}
        self.second = {}

    def dot(self, ka, la):
        tall = 3 * self.width
        lhs = self.lefts[1 + ka].reshape(tall, self.lefts.shape[3])
        rhs = self.rights[1 + la].reshape(tall, self.rights.shape[3])
        return lax.dot_general(lhs, rhs, (((1,), (1,)), ((), ())), preferred_element_type=jnp.float32)

    def cut(self, value, kb, lb):
        w = self.width
        return value[(kb + 1) * w:(kb + 2) * w, (lb + 1) * w:(lb + 2) * w]

    def compute_sent(self, side):
        ka = self.outer if side else -self.outer
        for la, pairs in ((ka, self.A_PAIRS), (0, self.B_PAIRS)):
            value = self.dot(ka, la)
            for at, kb, lb in pairs:
                self.out[side, at] = self.cut(value, kb, lb).astype(jnp.bfloat16)

    def start(self, side, chunk):
        da = -self.outer if side else self.outer
        at = self.CHUNKS[chunk]
        self.first[side, chunk] = self.wire(self.out.at[side, at], self.into.at[side, at], self.places.home(da, 0))

    def compute_own(self):
        for q, la in enumerate((0, -self.outer, self.outer)):
            value = self.dot(0, la)
            for at, kb, lb in (self.B_PAIRS if q else self.A_PAIRS):
                self.own[q, at] = self.cut(value, kb, lb)

    def total(self, q, at):
        value = self.own[q, at]
        for side in ((0, 1) if q == 0 else (q - 1,)):
            value = value + self.into[side, at].astype(jnp.float32)
        return value

    def forward(self, chunk):
        for side in (0, 1):
            self.first[side, chunk].wait_recv()
        base = 4 * chunk
        spots = [(0, base), (0, base + 1), (1, base + 2), (1, base + 3), (2, base + 2), (2, base + 3)]
        for at, (q, spot) in enumerate(spots):
            self.out_far[chunk, at] = self.total(q, spot).astype(jnp.bfloat16)

    def start_far(self, chunk):
        db = 1 if chunk else -1
        src, dst = self.out_far.at[chunk], self.into_far.at[chunk]
        if self.out_mid is None:
            self.second[chunk] = self.wire(src, dst, self.places.home(0, db))
        else:
            self.second[chunk] = self.wire(src, dst, self.places.inward(db), self.places.apart(db))

    def settle(self):
        for side in (0, 1):
            self.first[side, 2].wait_recv()

    def start_middle(self):
        for at, (q, spot) in enumerate(self.MIDDLE):
            self.out_mid[at] = self.total(q, spot).astype(jnp.bfloat16)
        self.second[2] = self.wire(
            self.out_mid, self.into_mid, self.places.inward(0), self.places.apart(0)
        )

    def middle(self, q, spot):
        if self.out_mid is None:
            return self.total(q, spot)
        return self.into_mid[self.MIDDLE.index((q, spot))].astype(jnp.float32)

    def finish(self, emit):
        for copy in self.second.values():
            copy.wait_recv()

        def far(chunk, at):
            return self.into_far[chunk, at].astype(jnp.float32)

        emit(0, 0, self.middle(0, 8) + far(0, 0) + far(1, 0))
        emit(0, 1, self.middle(0, 5) + far(0, 1))
        emit(0, -1, (self.middle(0, 1) + far(1, 1)).T)
        for q, pa in ((1, self.outer), (2, -self.outer)):
            emit(pa, 0, self.middle(q, 10) + far(0, 2 * q) + far(1, 2 * q))
            emit(pa, 1, self.middle(q, 9) + far(0, 2 * q + 1))
            emit(pa, -1, self.middle(q, 11) + far(1, 2 * q + 1))


def prepare(orb, pot, lefts, rights):
    width, cells = orb.shape[-2], orb.shape[-1]
    lane = lax.broadcasted_iota(jnp.int32, (width, 128), 1)
    for ka in range(3):
        for kb in range(3):
            source = orb[ka, kb]
            value = source.astype(jnp.float32)
            lefts[ka, kb, :, :cells] = source
            rights[ka, kb, :, :cells] = (value * pot[0]).astype(jnp.bfloat16)
            for line in range(cells // 128):
                piece = value[:, line * 128:(line + 1) * 128]
                ahead = pltpu.roll(piece, 127, 1)
                step = jnp.where(lane < 127, ahead - piece, 0.0).astype(jnp.bfloat16)
                at = cells + line * 128
                rights[ka, kb, :, at:at + 128] = step
                lefts[ka, kb, :, at:at + 128] = (step.astype(jnp.float32) * 0.5).astype(jnp.bfloat16)


def kernel(counts, orb_in, pot_in, den_in, pattern, ham, mar, pur,
           v_near, d_near, f_near, g_near, m_near, u_near, lefts, rights,
           s_own, s_out, s_into, s_far, s_back, h_own, h_out, h_into, h_far, h_back,
           s_mid, s_core, v_base, d_base, u_base,
           u_col, t_col, d_col, d_row, o_col, o_row, orb, pot, den, ham_own, mar_own, pur_own, sums, load, send, recv):
    width = orb.shape[-2]
    places = Places(counts)

    def keep(pa, pb):
        return pattern[3 * (1 + pa) + 1 + pb].astype(jnp.float32)

    loads = [
        pltpu.make_async_copy(src, dst, load.at[at])
        for at, (src, dst) in enumerate(((orb_in, orb), (den_in, den), (pot_in, pot)))
    ]
    for copy in loads:
        copy.start()
    barrier = pltpu.get_barrier_semaphore()
    greeted = places.greet(barrier)

    wire = Wire(send, recv)
    s_sum = Gram(wire, places, orb, orb, s_own, s_out, s_into, s_far, s_back, s_mid, s_core)
    h_sum = Gram(wire, places, lefts, rights, h_own, h_out, h_into, h_far, h_back)
    fields = Halo(wire, places, v_near, v_base, whole=True)
    density = Halo(wire, places, d_near, d_base)
    firsts = Halo(wire, places, f_near, split=True)
    seconds = Halo(wire, places, g_near, split=True)
    margin = Slim(wire, places, u_near)

    loads[0].wait()
    s_sum.compute_sent(0)
    loads[1].wait()
    loads[2].wait()
    for pa in SPAN:
        for pb in SPAN:
            at = 3 * pa + pb + 4
            v_base[at:at + 1] = jnp.full((1, 128), keep(pa, pb), jnp.float32)
            block = den[pa + 1, pb + 1].astype(jnp.float32) * keep(pa, pb)
            d_base[pa + 1, pb + 1] = block.astype(jnp.bfloat16)
    pl.semaphore_wait(barrier, greeted)

    for chunk in (0, 1):
        s_sum.start(0, chunk)
    fields.start_far()
    density.start_far()
    s_sum.start(0, 2)
    s_sum.compute_sent(1)
    for chunk in (0, 1, 2):
        s_sum.start(1, chunk)
    s_sum.compute_own()
    prepare(orb, pot, lefts, rights)
    for side in (0, 1):
        h_sum.compute_sent(side)
    h_sum.compute_own()
    fields.relay()
    for chunk in (0, 1):
        s_sum.forward(chunk)
        s_sum.start_far(chunk)
    density.relay(0, 3)
    s_sum.settle()
    s_sum.start_middle()
    density.relay(3)
    for side in (0, 1):
        h_sum.start(side, 0)
    fields.finish()

    def mask(ja, jb, pa, pb):
        at = 3 * (1 + pa) + 1 + pb
        return v_near[1 + ja, 1 + jb, pl.ds(at, 1), :width]

    def put_margin(a, b, value):
        m_near[1, 1, 1 + a, 1 + b] = (value * mask(0, 0, a, b)).astype(jnp.bfloat16)
        u_near[1, 1, 1 + a, 1 + b] = value.astype(jnp.bfloat16)
        u_col[1 + a, 1 + b] = (value * mask(a, b, -a, -b)).astype(jnp.bfloat16)

    s_sum.finish(put_margin)
    density.finish()

    def put_first(a, b, value):
        f_near[1, 1, 1 + a, 1 + b] = (value * mask(a, b, -a, -b)).astype(jnp.bfloat16)

    rows = groups(places.outer)
    for at, (ka, fas) in enumerate(rows):
        give(width, ka, column(
            width,
            lambda k, f: d_near[1 + k[0], 1 + k[1], 1 + f[0] - k[0], 1 + f[1] - k[1]],
            lambda f: u_col[1 + f[0], 1 + f[1]],
            True, ka, fas,
        ), put_first)
        firsts.ready(at)
    firsts.relay(0, 2)
    firsts.cross()
    firsts.relay(2)
    margin.start_far()
    margin.start_near()
    h_sum.forward(0)
    h_sum.start_far(0)

    def complete(local):
        for ja, jb in AROUND:
            for ka in SPAN:
                for kb in SPAN:
                    pa, pb = ka - ja, kb - jb
                    if abs(pa) > 1 or abs(pb) > 1 or local != ((ka, kb) == (0, 0)):
                        continue
                    if not local and Slim.sent(ja, jb, pa, pb):
                        block = u_near[ja + 1, jb + 1, pa + 1, pb + 1].astype(jnp.float32)
                    else:
                        block = u_near[ka + 1, kb + 1, 1 - pa, 1 - pb].astype(jnp.float32).T
                    kept = block * mask(ja, jb, pa, pb)
                    m_near[ja + 1, jb + 1, pa + 1, pb + 1] = kept.astype(jnp.bfloat16)

    complete(True)

    def put_third(a, b, value):
        kept = value * mask(a, b, -a, -b)
        pur_own[1 + a, 1 + b] = 3.0 * kept
        t_col[1 + a, 1 + b] = kept.astype(jnp.bfloat16)

    def finish_step(lefts_at, out, send):
        for at, (ka, fas) in enumerate(rows):
            def put_fifth(a, b, value):
                kept = value * mask(a, b, -a, -b)
                out[1 + a, 1 + b] = (pur_own[1 + a, 1 + b] - 2.0 * kept).astype(jnp.bfloat16)

            give(width, ka, column(
                width, lefts_at, lambda f: t_col[1 + f[0], 1 + f[1]], False, ka, fas
            ), put_fifth)
            for kb in SPAN:
                send(at, ka, kb)

    def first_at(k, f):
        return f_near[1 + f[0], 1 + f[1], 1 + k[0] - f[0], 1 + k[1] - f[1]]

    def density_at(f):
        return d_near[1 + f[0], 1 + f[1], 1 - f[0], 1 - f[1]]

    firsts.finish_inner()
    outer = places.outer
    sums[0] = column(width, first_at, density_at, False, outer, (0,))
    sums[1] = column(width, first_at, density_at, False, 0, (0, -outer))
    give(width, -outer, column(width, first_at, density_at, False, -outer, (0, -outer)), put_third)
    firsts.finish_outer()
    for at, ka in enumerate((outer, 0)):
        give(width, ka, column(width, first_at, density_at, False, ka, (outer,), sums[at]), put_third)

    turned = []

    def send_turn(at, a, b):
        if at == 1 and b == 0:
            d_row[1, 1] = d_col[1, 1]
        else:
            turned.append(wire(d_col.at[1 + a, 1 + b], d_row.at[1 - a, 1 - b], places.near(a, b)))

    finish_step(first_at, d_col, send_turn)
    margin.relay()
    back = wire(u_near.at[1, 1], u_base, places.outward(0, 0), places.away(0))
    for side in (0, 1):
        h_sum.start(side, 1)
    margin.finish()
    complete(False)
    for copy in turned:
        copy.wait_recv()

    def put_second(a, b, value):
        g_near[1, 1, 1 + a, 1 + b] = (value * mask(0, 0, a, b)).astype(jnp.bfloat16)

    product(d_row, m_near, outer, put_second, seconds.ready)
    seconds.relay(0, 2)
    seconds.cross()
    seconds.relay(2)
    for side in (0, 1):
        h_sum.start(side, 2)
    h_sum.forward(1)
    h_sum.start_far(1)
    def second_at(k, f):
        return g_near[1 + k[0], 1 + k[1], 1 + f[0] - k[0], 1 + f[1] - k[1]]

    def purer_at(f):
        return d_col[1 + f[0], 1 + f[1]]

    seconds.finish_inner()
    for ka, fas in (rows[1], rows[2]):
        give(width, ka, column(width, second_at, purer_at, False, ka, fas), put_third)
    seconds.finish_outer()
    give(width, outer, column(width, second_at, purer_at, False, *rows[0]), put_third)
    turned_out = []

    def send_out(at, a, b):
        turned_out.append(wire(
            o_col.at[1 + a, 1 + b], o_row.at[1 - a, 1 - b], places.outward(a, b),
            places.away(b) if at == 1 else None,
        ))

    finish_step(second_at, o_col, send_out)

    def put_ham(a, b, value):
        ham_own[1 + a, 1 + b] = value * keep(a, b)

    h_sum.settle()
    h_sum.finish(put_ham)
    saves = [
        pltpu.make_async_copy(src, dst, load.at[3 + at])
        for at, (src, dst) in enumerate(((ham_own, ham), (mar_own, mar), (pur_own, pur)))
    ]
    saves[0].start()
    back.wait_recv()
    for a, b in AROUND + [(0, 0)]:
        mar_own[1 + a, 1 + b] = u_base[1 + a, 1 + b].astype(jnp.float32) * keep(a, b)
    saves[1].start()
    for copy in turned_out:
        copy.wait_recv()
    for a in range(3):
        for b in range(3):
            pur_own[a, b] = o_row[a, b].astype(jnp.float32)
    saves[2].start()
    wire.drain()
    for copy in saves:
        copy.wait()


def store(*refs):
    count = (len(refs) - 1) // 3
    loads, saves = (
        [
            pltpu.make_async_copy(src, dst, refs[-1].at[base + at])
            for at, (src, dst) in enumerate(zip(srcs, dsts))
        ]
        for base, srcs, dsts in (
            (0, refs[:count], refs[2 * count:-1]), (count, refs[2 * count:-1], refs[count:2 * count])
        )
    )
    for copy in loads:
        copy.start()
    for one, other in zip(loads, saves):
        one.wait()
        other.start()
    for copy in saves:
        copy.wait()


def body(counts, orbitals, potential, density, pattern):
    width, cells = orbitals.shape[3], orbitals.shape[4]
    low = jnp.bfloat16
    near = pltpu.VMEM((3, 3, 3, 3, width, width), low)
    some = pltpu.VMEM((3, 3, width, width), low)
    blocks = jax.ShapeDtypeStruct((3, 3, width, width), jnp.float32)
    vmem = pl.BlockSpec(memory_space=pltpu.VMEM)
    pairs = [
        pltpu.VMEM((3, 12, width, width), jnp.float32),
        pltpu.VMEM((2, 12, width, width), low),
        pltpu.VMEM((2, 12, width, width), low),
        pltpu.VMEM((2, 6, width, width), low),
        pltpu.VMEM((2, 6, width, width), low),
    ]
    outs = pl.pallas_call(
        functools.partial(kernel, counts),
        out_shape=(blocks,) * 3,
        in_specs=[pl.BlockSpec(memory_space=pl.ANY)] * 3 + [pl.BlockSpec(memory_space=pltpu.SMEM)],
        out_specs=(pl.BlockSpec(memory_space=pltpu.HBM),) * 3,
        scratch_shapes=[
            pltpu.VMEM((3, 3, 16, 128), jnp.float32),
            near, near, near, near, near,
            pltpu.VMEM((3, 3, width, 2 * cells), low),
            pltpu.VMEM((3, 3, width, 2 * cells), low),
            *pairs, *pairs,
            pltpu.VMEM((9, width, width), low),
            pltpu.VMEM((9, width, width), low),
            pltpu.VMEM((16, 128), jnp.float32),
            some, some,
            some, some, some, some, some, some,
            pltpu.VMEM((3, 3, width, cells), low),
            pltpu.VMEM((1, 1, cells), jnp.float32),
            some,
            *[pltpu.VMEM((3, 3, width, width), jnp.float32)] * 3,
            pltpu.VMEM((2, 3 * width, width), jnp.float32),
            pltpu.SemaphoreType.DMA((6,)),
            pltpu.SemaphoreType.DMA((PORTS,)),
            pltpu.SemaphoreType.DMA((PORTS,)),
        ],
        compiler_params=pltpu.CompilerParams(
            collective_id=0, has_side_effects=True, vmem_limit_bytes=60 * 2**20
        ),
    )(
        orbitals.reshape(3, 3, width, cells),
        potential.reshape(1, 1, cells),
        density.reshape(3, 3, width, width),
        pattern.reshape(9),
    )
    outs = pl.pallas_call(
        store,
        out_shape=(blocks,) * 3,
        in_specs=[pl.BlockSpec(memory_space=pl.ANY)] * 3,
        out_specs=[pl.BlockSpec(memory_space=pltpu.HBM)] * 3,
        scratch_shapes=[pltpu.VMEM((3, 3, width, width), jnp.float32)] * 3
        + [pltpu.SemaphoreType.DMA((6,))],
        compiler_params=pltpu.CompilerParams(vmem_limit_bytes=60 * 2**20),
    )(*outs)
    return tuple(out.reshape(1, 1, 9, width, width) for out in outs)


def solution(mesh):
    rows = P("gx", "yz", None, None, None)
    flat = P("gx", "yz", None)
    return jax.shard_map(
        functools.partial(body, (mesh.shape["gx"], mesh.shape["yz"])),
        mesh=mesh,
        in_specs=(rows, flat, rows, flat),
        out_specs=(rows,) * 3,
        check_vma=False,
    )
```

```python
import functools

import jax
import jax.numpy as jnp
from jax import lax
from jax.experimental import pallas as pl
from jax.experimental.pallas import tpu as pltpu
from jax.sharding import PartitionSpec as P

MESH = pl.DeviceIdType.MESH
SPAN = (-1, 0, 1)
AROUND = [(a, b) for a in SPAN for b in SPAN if (a, b) != (0, 0)]
PORTS = 144


def part(d):
    return pl.ds(1, 2) if d == 1 else pl.ds(0, 2) if d == -1 else pl.ds(0, 3)


class Either:
    def __init__(self, copy, apart):
        self.copy, self.apart = copy, apart

    def wait_recv(self):
        pl.when(self.apart)(lambda: self.copy.wait_recv())

    def wait_send(self):
        pl.when(self.apart)(lambda: self.copy.wait_send())


class Wire:
    def __init__(self, send, recv):
        self.send, self.recv = send, recv
        self.ports = iter(range(PORTS))
        self.started = []

    def __call__(self, src, dst, device, apart=None):
        at = next(self.ports)
        copy = pltpu.make_async_remote_copy(
            src_ref=src, dst_ref=dst, send_sem=self.send.at[at], recv_sem=self.recv.at[at],
            device_id=device, device_id_type=MESH,
        )
        if apart is None:
            copy.start()
        else:
            pl.when(apart)(lambda: copy.start())

            @pl.when(jnp.logical_not(apart))
            def _():
                dst[...] = src[...]

            copy = Either(copy, apart)
        self.started.append(copy)
        return copy

    def drain(self):
        for copy in self.started:
            copy.wait_send()


class Places:
    def __init__(self, counts):
        self.counts = counts
        many = counts[1]
        self.table = list(range(many))
        if many % 2 == 0 and many >= 8:
            tall = many // 2
            self.table = [2, 0] + [2 * z + 1 for z in range(tall)] + [2 * z for z in range(tall - 1, 1, -1)]
        self.roles = [self.table.index(b) for b in range(many)]
        self.a, self.b = lax.axis_index("gx"), lax.axis_index("yz")
        self.c = self.pick(self.roles, self.b)
        self.outer = 2 * lax.rem(self.a, 2) - 1

    def pick(self, table, at):
        value = jnp.int32(table[0])
        for i in range(1, len(table)):
            value = jnp.where(at == i, jnp.int32(table[i]), value)
        return value

    def row(self, da):
        return lax.rem(self.a + da + self.counts[0], self.counts[0])

    def ring(self, b):
        return lax.rem(b + self.counts[1], self.counts[1])

    def seat(self, b):
        return self.pick(self.table, self.ring(b))

    def home(self, da, db):
        return self.row(da), self.ring(self.b + db)

    def near(self, da, db):
        return self.row(da), self.seat(self.c + db)

    def inward(self, db):
        return self.a, self.seat(self.b + db)

    def apart(self, db):
        return self.ring(self.b + db) != self.c

    def outward(self, da, db):
        return self.row(da), self.ring(self.c + db)

    def away(self, db):
        return self.ring(self.c + db) != self.b

    def greet(self, barrier):
        many = self.counts[1]
        lists = []
        for b in range(many):
            c, met = self.roles[b], set()
            for db in SPAN:
                met |= {(b + db) % many, self.table[(b + db) % many]}
                met |= {(c + db) % many, self.table[(c + db) % many]}
            lists.append(sorted(met - {b}))
        for at in range(max(len(met) for met in lists)):
            to = self.pick([met[at] if at < len(met) else -1 for met in lists], self.b)

            @pl.when(to >= 0)
            def _():
                for da in SPAN:
                    pl.semaphore_signal(
                        barrier, inc=1, device_id=(self.row(da), to), device_id_type=MESH
                    )

        for da in (1, -1):
            pl.semaphore_signal(barrier, inc=1, device_id=(self.row(da), self.b), device_id_type=MESH)
        return self.pick([3 * len(met) + 2 for met in lists], self.b)


class Halo:
    def __init__(self, wire, places, near, base=None, whole=False, split=False):
        self.wire, self.places, self.near, self.base = wire, places, near, base
        self.whole, self.split = whole, split
        outer = places.outer
        self.order = [
            (db, piece, pa, das)
            for piece, pa, das in (
                ((0, None, (1, -1)),) if whole else (
                    (0, 1, (outer, -outer)),
                    (2, 1 - outer, (-outer,)),
                    (1, 1 + outer, () if split else (outer,)),
                )
            )
            for db in ((1, -1) if base is None else (0, 1, -1))
        ]
        self.direct = {}
        self.passed = []

    def make(self, src, da, db, device, pa, apart=None):
        dst = self.near.at[1 - da, 1 - db]
        if not self.whole:
            src = src.at[pa, part(db)]
            dst = dst.at[pa, part(db)]
        return self.wire(src, dst, device, apart)

    def start_far(self, which=None):
        for db, piece, pa, _ in self.order:
            if which is not None and piece != which:
                continue
            if self.base is None:
                copy = self.make(self.near.at[1, 1], 0, db, self.places.near(0, db), pa)
            else:
                copy = self.make(self.base, 0, db, self.places.inward(db), pa, self.places.apart(db))
            self.direct[db, piece] = copy

    def start_near(self, name):
        outer = self.places.outer
        da, pa = {
            "turned": (outer, 1 + outer), "outer": (outer, 1),
            "inner": (-outer, 1), "last": (-outer, 1 - outer),
        }[name]
        self.direct[name] = self.make(self.near.at[1, 1], da, 0, self.places.near(da, 0), pa)

    def ready(self, at):
        if at == 0:
            self.start_near("turned")
        elif at == 1:
            self.start_far(0)
            self.start_near("outer")
            self.start_near("inner")
        else:
            self.start_far(2)
            self.start_far(1)
            self.start_near("last")

    def relay(self, start=0, stop=None):
        for db, piece, pa, das in self.order[start:stop]:
            if das:
                self.direct[db, piece].wait_recv()
            for at, da in enumerate(das):
                src = self.near.at[1, 1 - db]
                copy = self.make(src, da, db, self.places.near(da, 0), pa)
                self.passed.append((piece == 2 or at == 1, copy))

    def cross(self):
        outer = self.places.outer
        self.direct["turned"].wait_recv()
        for db in (1, -1):
            src = self.near.at[1 + outer, 1, 1 - outer, part(db)]
            dst = self.near.at[1 + outer, 1 - db, 1 - outer, part(db)]
            self.passed.append((False, self.wire(src, dst, self.places.near(0, db))))

    def finish_inner(self):
        for db, piece, _, das in self.order:
            if not das:
                self.direct[db, piece].wait_recv()
        for name in ("inner", "last"):
            self.direct[name].wait_recv()
        for inner, copy in self.passed:
            if inner:
                copy.wait_recv()

    def finish_outer(self):
        self.direct["outer"].wait_recv()
        for inner, copy in self.passed:
            if not inner:
                copy.wait_recv()

    def finish(self):
        for _, copy in self.passed:
            copy.wait_recv()


class Slim:
    def __init__(self, wire, places, near):
        self.wire, self.places, self.near = wire, places, near
        self.far, self.close, self.passed = {}, [], []

    def start_far(self):
        own = self.near.at[1, 1]
        for db in (1, -1):
            dst = self.near.at[1, 1 - db]
            self.far[db] = self.wire(
                own.at[pl.ds(0, 3), 1], dst.at[pl.ds(0, 3), 1], self.places.near(0, db)
            )

    def start_near(self):
        own = self.near.at[1, 1]
        for da in (1, -1):
            dst = self.near.at[1 - da, 1]
            to = self.places.near(da, 0)
            self.close.append(self.wire(own.at[1], dst.at[1], to))
            for pb in (0, 2):
                self.close.append(self.wire(own.at[1 + da, pb], dst.at[1 + da, pb], to))

    def relay(self):
        for db in (1, -1):
            self.far[db].wait_recv()
            for da in (1, -1):
                src = self.near.at[1, 1 - db, 1, 1]
                dst = self.near.at[1 - da, 1 - db, 1, 1]
                self.passed.append(self.wire(src, dst, self.places.near(da, 0)))

    def finish(self):
        for copy in self.close + self.passed:
            copy.wait_recv()

    @staticmethod
    def sent(ja, jb, pa, pb):
        if (pa, pb) == (0, 0):
            return True
        if ja == 0:
            return pb == 0
        return jb == 0 and pb != 0 and pa in (0, -ja)


def groups(outer):
    return ((outer, (0, outer)), (0, (0, outer, -outer)), (-outer, (0, -outer)))


def product(left, near, outer, emit, done):
    width = left.shape[-1]
    blank = jnp.zeros((width, width), jnp.bfloat16)
    for pa, fas in groups(outer):
        total = None
        for fa in fas:
            lhs = jnp.concatenate([left[fa + 1, fb + 1] for fb in SPAN], axis=1)
            rhs = jnp.concatenate([
                jnp.concatenate([
                    near[fa + 1, fb + 1, pa - fa + 1, pb - fb + 1] if abs(pb - fb) <= 1 else blank
                    for pb in SPAN
                ], axis=1) for fb in SPAN
            ], axis=0)
            term = jnp.dot(lhs, rhs, preferred_element_type=jnp.float32)
            total = term if total is None else total + term
        for pb in SPAN:
            emit(pa, pb, total[:, (pb + 1) * width:(pb + 2) * width])
    for at in range(3):
        done(at)


def column(width, lefts, rights, turned, ka, fas, base=None):
    blank = jnp.zeros((width, width), jnp.bfloat16)
    inner = [(fa, fb) for fa in fas for fb in SPAN]
    lhs = jnp.concatenate([
        jnp.concatenate(
            [lefts((ka, kb), f) if abs(f[1] - kb) <= 1 else blank for f in inner], axis=1
        ) for kb in SPAN
    ], axis=0)
    rhs = jnp.concatenate([rights(f) for f in inner], axis=1 if turned else 0)
    total = lax.dot_general(
        lhs, rhs, (((1,), (1 if turned else 0,)), ((), ())), preferred_element_type=jnp.float32
    )
    return total if base is None else total + base


def give(width, ka, total, emit):
    for kb in SPAN:
        emit(ka, kb, total[(kb + 1) * width:(kb + 2) * width])


class Gram:
    A_PAIRS = ((0, 1, 1), (1, 1, 0), (4, -1, -1), (5, 0, -1), (8, 0, 0))
    B_PAIRS = ((2, 1, 1), (3, 1, 0), (6, -1, -1), (7, -1, 0), (9, 0, -1), (10, 0, 0), (11, 0, 1))
    MIDDLE = ((0, 8), (0, 5), (0, 1), (1, 9), (1, 10), (1, 11), (2, 9), (2, 10), (2, 11))
    CHUNKS = (pl.ds(0, 4), pl.ds(4, 4), pl.ds(8, 4))

    def __init__(self, wire, places, lefts, rights, own, out, into, out_far, into_far, out_mid=None, into_mid=None):
        self.wire, self.places, self.outer = wire, places, places.outer
        self.lefts, self.rights = lefts, rights
        self.own, self.out, self.into, self.out_far, self.into_far = own, out, into, out_far, into_far
        self.out_mid, self.into_mid = out_mid, into_mid
        self.width = lefts.shape[2]
        self.first = {}
        self.second = {}

    def dot(self, ka, la):
        tall = 3 * self.width
        lhs = self.lefts[1 + ka].reshape(tall, self.lefts.shape[3])
        rhs = self.rights[1 + la].reshape(tall, self.rights.shape[3])
        return lax.dot_general(lhs, rhs, (((1,), (1,)), ((), ())), preferred_element_type=jnp.float32)

    def cut(self, value, kb, lb):
        w = self.width
        return value[(kb + 1) * w:(kb + 2) * w, (lb + 1) * w:(lb + 2) * w]

    def compute_sent(self, side):
        ka = self.outer if side else -self.outer
        for la, pairs in ((ka, self.A_PAIRS), (0, self.B_PAIRS)):
            value = self.dot(ka, la)
            for at, kb, lb in pairs:
                self.out[side, at] = self.cut(value, kb, lb).astype(jnp.bfloat16)

    def start(self, side, chunk):
        da = -self.outer if side else self.outer
        at = self.CHUNKS[chunk]
        self.first[side, chunk] = self.wire(self.out.at[side, at], self.into.at[side, at], self.places.home(da, 0))

    def compute_own(self):
        for q, la in enumerate((0, -self.outer, self.outer)):
            value = self.dot(0, la)
            for at, kb, lb in (self.B_PAIRS if q else self.A_PAIRS):
                self.own[q, at] = self.cut(value, kb, lb)

    def total(self, q, at):
        value = self.own[q, at]
        for side in ((0, 1) if q == 0 else (q - 1,)):
            value = value + self.into[side, at].astype(jnp.float32)
        return value

    def forward(self, chunk):
        for side in (0, 1):
            self.first[side, chunk].wait_recv()
        base = 4 * chunk
        spots = [(0, base), (0, base + 1), (1, base + 2), (1, base + 3), (2, base + 2), (2, base + 3)]
        for at, (q, spot) in enumerate(spots):
            self.out_far[chunk, at] = self.total(q, spot).astype(jnp.bfloat16)

    def start_far(self, chunk):
        db = 1 if chunk else -1
        src, dst = self.out_far.at[chunk], self.into_far.at[chunk]
        if self.out_mid is None:
            self.second[chunk] = self.wire(src, dst, self.places.home(0, db))
        else:
            self.second[chunk] = self.wire(src, dst, self.places.inward(db), self.places.apart(db))

    def settle(self):
        for side in (0, 1):
            self.first[side, 2].wait_recv()

    def start_middle(self):
        for at, (q, spot) in enumerate(self.MIDDLE):
            self.out_mid[at] = self.total(q, spot).astype(jnp.bfloat16)
        self.second[2] = self.wire(
            self.out_mid, self.into_mid, self.places.inward(0), self.places.apart(0)
        )

    def middle(self, q, spot):
        if self.out_mid is None:
            return self.total(q, spot)
        return self.into_mid[self.MIDDLE.index((q, spot))].astype(jnp.float32)

    def finish(self, emit):
        for copy in self.second.values():
            copy.wait_recv()

        def far(chunk, at):
            return self.into_far[chunk, at].astype(jnp.float32)

        emit(0, 0, self.middle(0, 8) + far(0, 0) + far(1, 0))
        emit(0, 1, self.middle(0, 5) + far(0, 1))
        emit(0, -1, (self.middle(0, 1) + far(1, 1)).T)
        for q, pa in ((1, self.outer), (2, -self.outer)):
            emit(pa, 0, self.middle(q, 10) + far(0, 2 * q) + far(1, 2 * q))
            emit(pa, 1, self.middle(q, 9) + far(0, 2 * q + 1))
            emit(pa, -1, self.middle(q, 11) + far(1, 2 * q + 1))


def prepare(orb, pot, lefts, rights):
    width, cells = orb.shape[-2], orb.shape[-1]
    lane = lax.broadcasted_iota(jnp.int32, (width, 128), 1)
    for ka in range(3):
        for kb in range(3):
            source = orb[ka, kb]
            value = source.astype(jnp.float32)
            lefts[ka, kb, :, :cells] = source
            rights[ka, kb, :, :cells] = (value * pot[0]).astype(jnp.bfloat16)
            for line in range(cells // 128):
                piece = value[:, line * 128:(line + 1) * 128]
                ahead = pltpu.roll(piece, 127, 1)
                step = jnp.where(lane < 127, ahead - piece, 0.0).astype(jnp.bfloat16)
                at = cells + line * 128
                rights[ka, kb, :, at:at + 128] = step
                lefts[ka, kb, :, at:at + 128] = (step.astype(jnp.float32) * 0.5).astype(jnp.bfloat16)


def kernel(counts, orb_in, pot_in, den_in, pattern, ham, mar, pur,
           v_near, d_near, f_near, g_near, m_near, u_near, lefts, rights,
           s_own, s_out, s_into, s_far, s_back, h_own, h_out, h_into, h_far, h_back,
           s_mid, s_core, v_base, d_base, u_base,
           u_col, t_col, d_col, d_row, o_col, o_row, orb, pot, den, ham_own, mar_own, pur_own, sums, load, send, recv):
    width = orb.shape[-2]
    places = Places(counts)

    def keep(pa, pb):
        return pattern[3 * (1 + pa) + 1 + pb].astype(jnp.float32)

    loads = [
        pltpu.make_async_copy(src, dst, load.at[at])
        for at, (src, dst) in enumerate(((orb_in, orb), (den_in, den), (pot_in, pot)))
    ]
    for copy in loads:
        copy.start()
    barrier = pltpu.get_barrier_semaphore()
    greeted = places.greet(barrier)

    wire = Wire(send, recv)
    s_sum = Gram(wire, places, orb, orb, s_own, s_out, s_into, s_far, s_back, s_mid, s_core)
    h_sum = Gram(wire, places, lefts, rights, h_own, h_out, h_into, h_far, h_back)
    fields = Halo(wire, places, v_near, v_base, whole=True)
    density = Halo(wire, places, d_near, d_base)
    firsts = Halo(wire, places, f_near, split=True)
    seconds = Halo(wire, places, g_near, split=True)
    margin = Slim(wire, places, u_near)

    loads[0].wait()
    s_sum.compute_sent(0)
    loads[1].wait()
    loads[2].wait()
    for pa in SPAN:
        for pb in SPAN:
            at = 3 * pa + pb + 4
            v_base[at:at + 1] = jnp.full((1, 128), keep(pa, pb), jnp.float32)
            block = den[pa + 1, pb + 1].astype(jnp.float32) * keep(pa, pb)
            d_base[pa + 1, pb + 1] = block.astype(jnp.bfloat16)
    pl.semaphore_wait(barrier, greeted)

    for chunk in (0, 1):
        s_sum.start(0, chunk)
    fields.start_far()
    density.start_far()
    s_sum.start(0, 2)
    s_sum.compute_sent(1)
    for chunk in (0, 1, 2):
        s_sum.start(1, chunk)
    s_sum.compute_own()
    prepare(orb, pot, lefts, rights)
    for side in (0, 1):
        h_sum.compute_sent(side)
    h_sum.compute_own()
    fields.relay()
    for chunk in (0, 1):
        s_sum.forward(chunk)
        s_sum.start_far(chunk)
    density.relay(0, 3)
    s_sum.settle()
    s_sum.start_middle()
    density.relay(3)
    for side in (0, 1):
        h_sum.start(side, 0)
    fields.finish()

    def mask(ja, jb, pa, pb):
        at = 3 * (1 + pa) + 1 + pb
        return v_near[1 + ja, 1 + jb, pl.ds(at, 1), :width]

    def put_margin(a, b, value):
        m_near[1, 1, 1 + a, 1 + b] = (value * mask(0, 0, a, b)).astype(jnp.bfloat16)
        u_near[1, 1, 1 + a, 1 + b] = value.astype(jnp.bfloat16)
        u_col[1 + a, 1 + b] = (value * mask(a, b, -a, -b)).astype(jnp.bfloat16)

    s_sum.finish(put_margin)
    density.finish()

    def put_first(a, b, value):
        f_near[1, 1, 1 + a, 1 + b] = (value * mask(a, b, -a, -b)).astype(jnp.bfloat16)

    rows = groups(places.outer)
    for ka, fas in rows:
        give(width, ka, column(
            width,
            lambda k, f: d_near[1 + k[0], 1 + k[1], 1 + f[0] - k[0], 1 + f[1] - k[1]],
            lambda f: u_col[1 + f[0], 1 + f[1]],
            True, ka, fas,
        ), put_first)
    for at in range(3):
        firsts.ready(at)
    firsts.relay(0, 2)
    firsts.cross()
    margin.start_far()
    firsts.relay(2)
    margin.start_near()
    h_sum.forward(0)
    h_sum.start_far(0)

    def complete(local):
        for ja, jb in AROUND:
            for ka in SPAN:
                for kb in SPAN:
                    pa, pb = ka - ja, kb - jb
                    if abs(pa) > 1 or abs(pb) > 1 or local != ((ka, kb) == (0, 0)):
                        continue
                    if not local and Slim.sent(ja, jb, pa, pb):
                        block = u_near[ja + 1, jb + 1, pa + 1, pb + 1].astype(jnp.float32)
                    else:
                        block = u_near[ka + 1, kb + 1, 1 - pa, 1 - pb].astype(jnp.float32).T
                    kept = block * mask(ja, jb, pa, pb)
                    m_near[ja + 1, jb + 1, pa + 1, pb + 1] = kept.astype(jnp.bfloat16)

    complete(True)

    def put_third(a, b, value):
        kept = value * mask(a, b, -a, -b)
        pur_own[1 + a, 1 + b] = 3.0 * kept
        t_col[1 + a, 1 + b] = kept.astype(jnp.bfloat16)

    def finish_step(lefts_at, out, send):
        def put_fifth(a, b, value):
            kept = value * mask(a, b, -a, -b)
            out[1 + a, 1 + b] = (pur_own[1 + a, 1 + b] - 2.0 * kept).astype(jnp.bfloat16)

        for ka, fas in rows:
            give(width, ka, column(
                width, lefts_at, lambda f: t_col[1 + f[0], 1 + f[1]], False, ka, fas
            ), put_fifth)
        for at, (ka, _) in enumerate(rows):
            for kb in SPAN:
                send(at, ka, kb)

    def first_at(k, f):
        return f_near[1 + f[0], 1 + f[1], 1 + k[0] - f[0], 1 + k[1] - f[1]]

    def density_at(f):
        return d_near[1 + f[0], 1 + f[1], 1 - f[0], 1 - f[1]]

    firsts.finish_inner()
    outer = places.outer
    sums[0] = column(width, first_at, density_at, False, outer, (0,))
    sums[1] = column(width, first_at, density_at, False, 0, (0, -outer))
    give(width, -outer, column(width, first_at, density_at, False, -outer, (0, -outer)), put_third)
    firsts.finish_outer()
    for at, ka in enumerate((outer, 0)):
        give(width, ka, column(width, first_at, density_at, False, ka, (outer,), sums[at]), put_third)

    turned = []

    def send_turn(at, a, b):
        if at == 1 and b == 0:
            d_row[1, 1] = d_col[1, 1]
        else:
            turned.append(wire(d_col.at[1 + a, 1 + b], d_row.at[1 - a, 1 - b], places.near(a, b)))

    finish_step(first_at, d_col, send_turn)
    margin.relay()
    back = wire(u_near.at[1, 1], u_base, places.outward(0, 0), places.away(0))
    for side in (0, 1):
        h_sum.start(side, 1)
    margin.finish()
    complete(False)
    for copy in turned:
        copy.wait_recv()

    def put_second(a, b, value):
        g_near[1, 1, 1 + a, 1 + b] = (value * mask(0, 0, a, b)).astype(jnp.bfloat16)

    product(d_row, m_near, outer, put_second, seconds.ready)
    seconds.relay(0, 2)
    seconds.cross()
    seconds.relay(2)
    for side in (0, 1):
        h_sum.start(side, 2)
    h_sum.forward(1)
    h_sum.start_far(1)
    def second_at(k, f):
        return g_near[1 + k[0], 1 + k[1], 1 + f[0] - k[0], 1 + f[1] - k[1]]

    def purer_at(f):
        return d_col[1 + f[0], 1 + f[1]]

    seconds.finish_inner()
    for ka, fas in (rows[1], rows[2]):
        give(width, ka, column(width, second_at, purer_at, False, ka, fas), put_third)
    seconds.finish_outer()
    give(width, outer, column(width, second_at, purer_at, False, *rows[0]), put_third)
    turned_out = []

    def send_out(at, a, b):
        turned_out.append(wire(
            o_col.at[1 + a, 1 + b], o_row.at[1 - a, 1 - b], places.outward(a, b),
            places.away(b) if at == 1 else None,
        ))

    finish_step(second_at, o_col, send_out)

    def put_ham(a, b, value):
        ham_own[1 + a, 1 + b] = value * keep(a, b)

    h_sum.settle()
    h_sum.finish(put_ham)
    saves = [
        pltpu.make_async_copy(src, dst, load.at[3 + at])
        for at, (src, dst) in enumerate(((ham_own, ham), (mar_own, mar), (pur_own, pur)))
    ]
    saves[0].start()
    back.wait_recv()
    for a, b in AROUND + [(0, 0)]:
        mar_own[1 + a, 1 + b] = u_base[1 + a, 1 + b].astype(jnp.float32) * keep(a, b)
    saves[1].start()
    for copy in turned_out:
        copy.wait_recv()
    for a in range(3):
        for b in range(3):
            pur_own[a, b] = o_row[a, b].astype(jnp.float32)
    saves[2].start()
    wire.drain()
    for copy in saves:
        copy.wait()


def store(*refs):
    count = (len(refs) - 1) // 3
    loads, saves = (
        [
            pltpu.make_async_copy(src, dst, refs[-1].at[base + at])
            for at, (src, dst) in enumerate(zip(srcs, dsts))
        ]
        for base, srcs, dsts in (
            (0, refs[:count], refs[2 * count:-1]), (count, refs[2 * count:-1], refs[count:2 * count])
        )
    )
    for copy in loads:
        copy.start()
    for one, other in zip(loads, saves):
        one.wait()
        other.start()
    for copy in saves:
        copy.wait()


def body(counts, orbitals, potential, density, pattern):
    width, cells = orbitals.shape[3], orbitals.shape[4]
    low = jnp.bfloat16
    near = pltpu.VMEM((3, 3, 3, 3, width, width), low)
    some = pltpu.VMEM((3, 3, width, width), low)
    blocks = jax.ShapeDtypeStruct((3, 3, width, width), jnp.float32)
    vmem = pl.BlockSpec(memory_space=pltpu.VMEM)
    pairs = [
        pltpu.VMEM((3, 12, width, width), jnp.float32),
        pltpu.VMEM((2, 12, width, width), low),
        pltpu.VMEM((2, 12, width, width), low),
        pltpu.VMEM((2, 6, width, width), low),
        pltpu.VMEM((2, 6, width, width), low),
    ]
    outs = pl.pallas_call(
        functools.partial(kernel, counts),
        out_shape=(blocks,) * 3,
        in_specs=[pl.BlockSpec(memory_space=pl.ANY)] * 3 + [pl.BlockSpec(memory_space=pltpu.SMEM)],
        out_specs=(pl.BlockSpec(memory_space=pltpu.HBM),) * 3,
        scratch_shapes=[
            pltpu.VMEM((3, 3, 16, 128), jnp.float32),
            near, near, near, near, near,
            pltpu.VMEM((3, 3, width, 2 * cells), low),
            pltpu.VMEM((3, 3, width, 2 * cells), low),
            *pairs, *pairs,
            pltpu.VMEM((9, width, width), low),
            pltpu.VMEM((9, width, width), low),
            pltpu.VMEM((16, 128), jnp.float32),
            some, some,
            some, some, some, some, some, some,
            pltpu.VMEM((3, 3, width, cells), low),
            pltpu.VMEM((1, 1, cells), jnp.float32),
            some,
            *[pltpu.VMEM((3, 3, width, width), jnp.float32)] * 3,
            pltpu.VMEM((2, 3 * width, width), jnp.float32),
            pltpu.SemaphoreType.DMA((6,)),
            pltpu.SemaphoreType.DMA((PORTS,)),
            pltpu.SemaphoreType.DMA((PORTS,)),
        ],
        compiler_params=pltpu.CompilerParams(
            collective_id=0, has_side_effects=True, vmem_limit_bytes=60 * 2**20
        ),
    )(
        orbitals.reshape(3, 3, width, cells),
        potential.reshape(1, 1, cells),
        density.reshape(3, 3, width, width),
        pattern.reshape(9),
    )
    outs = pl.pallas_call(
        store,
        out_shape=(blocks,) * 3,
        in_specs=[pl.BlockSpec(memory_space=pl.ANY)] * 3,
        out_specs=[pl.BlockSpec(memory_space=pltpu.HBM)] * 3,
        scratch_shapes=[pltpu.VMEM((3, 3, width, width), jnp.float32)] * 3
        + [pltpu.SemaphoreType.DMA((6,))],
        compiler_params=pltpu.CompilerParams(vmem_limit_bytes=60 * 2**20),
    )(*outs)
    return tuple(out.reshape(1, 1, 9, width, width) for out in outs)


def solution(mesh):
    rows = P("gx", "yz", None, None, None)
    flat = P("gx", "yz", None)
    return jax.shard_map(
        functools.partial(body, (mesh.shape["gx"], mesh.shape["yz"])),
        mesh=mesh,
        in_specs=(rows, flat, rows, flat),
        out_specs=(rows,) * 3,
        check_vma=False,
    )
```
